32 devices in a mesh: member: 2 (over y), win: 4 (over z), seq: 4 (over x, core).
Axes of the slice: x: 2, y: 2, z: 4, core: 2. Of those that a mesh axis runs over, the one named last changes fastest.
Arguments:
- pixel_grid_input: bfloat16 [8, 8, 4, 64, 1536], P(('member', 'win'), None, 'seq'), parts along dimension 0, may hold values from -6 to 6
- mask_zone_labeling: int32 [8, 32, 64], P(('member', 'win')), parts along dimension 0, may hold values from 0 to 8, as said below
- standardize_multiplier: float32 [1536], replicated, may hold values from 0.25 to 1.75
- standardize_offset_vector: float32 [1536], replicated, may hold values from -3 to 3
- triple_projection_matrix: bfloat16 [3, 1536, 1536], P(None, None, 'seq'), may hold values from -0.15625 to 0.15625
- logit_scaling_per_part: float32 [16], P('seq'), may hold values from 1 to 45
- final_projection_matrix: bfloat16 [1536, 1536], P('seq'), may hold values from -0.15625 to 0.15625
Outputs:
- mixed: bfloat16 [8, 8, 4, 64, 1536], P(('member', 'win'), None, 'seq'), parts along dimension 0
The draws below stay inside these ranges and needn't reach their ends.
There are 2 independent parts, one for each index of `member`. The reference program is written for one: setup_inputs(seed, part) draws one part's arguments, and reference() takes and returns one part's arrays. A program takes and returns all parts, laid end to end along the dimension named above; an argument that names none is the same for every part. Nothing has to cross between parts.
Inputs may be any that keep to these rules, and one draw needn't show every extreme that they name: `mask_zone_labeling`: region is 3 * (row band) + (column band) of the pixel on the rolled grid: the row band is 0 in the first 32 rows, 1 in the next rows and 2 in the last few rows, whose count is drawn once for each member from 4 to 27; the column bands are cut the same way within the last 32 columns of the grid, with a count drawn apart. Only windows in the last window row or the last window column of the grid hold more than one region.
All inputs are finite; a program needn't handle non-finite values.
Results may differ from the reference program's by a relative error of at most 0.0065.
The reference program's roundings to bfloat16 on the way count: a program that leaves them out, or rounds other values in their place, can miss the bound.
Values may be sent and summed in bfloat16 or wider, within the bound.
A program may use at most 64 MiB of HBM per device.

```python
import math
import jax
import jax.numpy as jnp
from jax import lax

D = 1536
HEADS = 16
CHANNEL_PER_PART = 96
WS = 32
WCD = 2
SHIFT = 16
LANES = 4
AROWS = 8
COLS = 64
N_WIN = 4


def draw_logit_scaling_per_part(key, part):
    logs = jax.random.uniform(key, (HEADS,), jnp.float32, 0.0, jnp.log(6.0))
    return jnp.exp(logs)


def draw_mask_zone_labeling(key, part):
    cuts = jax.random.randint(jax.random.fold_in(key, 17), (2,), 4, WS - 4)
    row_cut = cuts[0]
    col_cut = cuts[1]
    grid_rows = 2 * WS
    grid_width = N_WIN // 2 * COLS
    block_index = lax.broadcasted_iota(jnp.int32, (N_WIN, WS, COLS), 0)
    inner_row = lax.broadcasted_iota(jnp.int32, (N_WIN, WS, COLS), 1)
    inner_col = lax.broadcasted_iota(jnp.int32, (N_WIN, WS, COLS), 2)
    grid_row = block_index % 2 * WS + inner_row
    grid_col = block_index // 2 * COLS + inner_col
    row_band = jnp.where(grid_row < WS, 0, jnp.where(grid_row < grid_rows - row_cut, 1, 2))
    col_band = jnp.where(grid_col < grid_width - WS, 0, jnp.where(grid_col < grid_width - col_cut, 1, 2))
    return (3 * row_band + col_band).astype(jnp.int32)


def block_levels(own_key, shape, split, smallest, largest):
    loudness, own = 1.0, jax.random.fold_in(own_key, 6)
    for dim, blocks in split:
        heights = jnp.exp(jax.random.uniform(jax.random.fold_in(own, dim), (blocks,), jnp.float32, smallest / len(split), largest / len(split)))
        loudness = loudness * jnp.repeat(heights, shape[dim] // blocks).reshape([-1 if axis == dim else 1 for axis in range(len(shape))])
    return loudness


def scatter_about(key, shape, scale, bound, shards=(), kind=jnp.bfloat16):
    factor_of = block_levels(key, shape, shards, -0.22, 0.18) if shards else 1.0
    entries = jax.random.normal(key, shape, jnp.float32) * scale * factor_of
    return jnp.minimum(jnp.maximum(entries, -bound), bound).astype(kind)


def setup_inputs(seed: int = 0, part: int = 0) -> dict:
    key_list = jax.random.split(jax.random.key(seed), 8)
    own_keys = jax.random.split(jax.random.fold_in(key_list[7], part), 8)
    pixel_grid_input = scatter_about(own_keys[0], (N_WIN, AROWS, LANES, COLS, D), 1.0, 6.0, ((0, 4), (2, 4)))
    mask_zone_labeling = draw_mask_zone_labeling(jax.random.fold_in(jax.random.fold_in(key_list[7], part), 71), part)
    standardize_multiplier = jnp.clip(1.0 + 0.15 * jax.random.normal(key_list[2], (D,), jnp.float32), 0.25, 1.75)
    standardize_offset_vector = scatter_about(key_list[3], (D,), 0.5, 3.0, (), jnp.float32)
    triple_projection_matrix = scatter_about(key_list[4], (3, D, HEADS * CHANNEL_PER_PART), D ** -0.5, 0.15625, ((2, 4),))
    logit_scaling_per_part = draw_logit_scaling_per_part(jax.random.fold_in(key_list[7], 71), part)
    final_projection_matrix = scatter_about(key_list[6], (HEADS * CHANNEL_PER_PART, D), (HEADS * CHANNEL_PER_PART) ** -0.5, 0.15625, ((0, 4),))
    return dict(pixel_grid_input=pixel_grid_input, mask_zone_labeling=mask_zone_labeling, standardize_multiplier=standardize_multiplier, standardize_offset_vector=standardize_offset_vector, triple_projection_matrix=triple_projection_matrix, logit_scaling_per_part=logit_scaling_per_part, final_projection_matrix=final_projection_matrix)


def layer_norm(values_in, gain_vector, bias_vector):
    values = values_in.astype(jnp.float32)
    average = lax.optimization_barrier(jnp.mean(values, axis=-1, keepdims=True))
    centred = values - average
    variance = lax.optimization_barrier(jnp.mean(centred * centred, axis=-1, keepdims=True))
    return (centred * lax.rsqrt(variance + 1e-05) * gain_vector + bias_vector).astype(jnp.bfloat16)

def window_attend(triple, labels, logit_multiplier):
    queries = triple[0].astype(jnp.float32)
    keys_all = triple[1].astype(jnp.float32)
    values_all = triple[2].astype(jnp.float32)
    scores = jnp.einsum('hpe,hke->hpk', queries, keys_all) * logit_multiplier[:, None, None]
    same_region = labels[:, None] == labels[None, :]
    scores = jnp.where(same_region[None], scores, -1e+30)
    row_max = lax.optimization_barrier(jnp.max(scores, axis=-1, keepdims=True))
    numerators = jnp.exp(scores - row_max)
    probabilities = (numerators / lax.optimization_barrier(jnp.sum(numerators, axis=-1, keepdims=True))).astype(jnp.bfloat16)
    return jnp.einsum('hpk,hke->hpe', probabilities.astype(jnp.float32), values_all).astype(jnp.bfloat16)

def reference(pixel_grid_input, mask_zone_labeling, standardize_multiplier, standardize_offset_vector, triple_projection_matrix, logit_scaling_per_part, final_projection_matrix):
    grid_cols = N_WIN // 2
    blocks = pixel_grid_input.reshape(grid_cols, 2, WS, COLS, D)
    image = blocks.transpose(1, 2, 0, 3, 4).reshape(2 * WS, grid_cols * COLS, D)
    image = jnp.roll(image, (-SHIFT, -SHIFT), axis=(0, 1))
    blocks = image.reshape(2, WS, grid_cols, COLS, D).transpose(2, 0, 1, 3, 4).reshape(N_WIN, WS, COLS, D)
    windows = blocks.reshape(N_WIN, WS, WCD, WS, D).transpose(0, 2, 1, 3, 4).reshape(N_WIN * WCD, WS * WS, D)
    labels = mask_zone_labeling.reshape(N_WIN, WS, WCD, WS).transpose(0, 2, 1, 3).reshape(N_WIN * WCD, WS * WS)
    weights_qkv = triple_projection_matrix.astype(jnp.float32)
    logit_multiplier = logit_scaling_per_part / math.sqrt(CHANNEL_PER_PART)

    def one_window(pair):
        tokens, token_region_labels = pair
        normed = layer_norm(tokens, standardize_multiplier, standardize_offset_vector)
        triple = jnp.einsum('pd,tdc->tpc', normed.astype(jnp.float32), weights_qkv).astype(jnp.bfloat16)
        triple = triple.reshape(3, WS * WS, HEADS, CHANNEL_PER_PART).transpose(0, 2, 1, 3)
        heads_out = window_attend(triple, token_region_labels, logit_multiplier)
        joined = heads_out.transpose(1, 0, 2).reshape(WS * WS, HEADS * CHANNEL_PER_PART)
        attention_update = jnp.dot(joined, final_projection_matrix, preferred_element_type=jnp.float32)
        return (tokens.astype(jnp.float32) + attention_update).astype(jnp.bfloat16)
    result = lax.map(one_window, (windows, labels))
    result = result.reshape(N_WIN, WCD, WS, WS, D).transpose(0, 2, 1, 3, 4)
    return result.reshape(N_WIN, AROWS, LANES, COLS, D)
```

```python
import functools
import math

import jax
import jax.numpy as jnp
from jax import lax
from jax.experimental import pallas as pl
from jax.experimental.pallas import tpu as pltpu
from jax.sharding import PartitionSpec as P

CHANNEL_PER_PART = 96
PADDED = 128
WS = 32
LOG2E = 1.4426950408889634


def norm_kernel(take, gain_ref, bias_ref, top_ref, *refs):
    pieces, pixels_ref, normed_ref = refs[:-2], refs[-2], refs[-1]
    first, last = take
    wide = last - first
    gain = gain_ref[...]
    offset = bias_ref[...]
    parts = [(0, 0, top_ref[:, first:last]), (1, 0, pieces[0][...])]
    if len(pieces) > 1:
        parts += [(0, wide, pieces[1][...]), (1, wide, pieces[2][...])]
    for place, start, part in parts:
        span = slice(start, start + part.shape[1])
        pixels_ref[place, :, span] = part
        values = part.astype(jnp.float32)
        average = jnp.mean(values, axis=-1, keepdims=True)
        centred = values - average
        variance = jnp.mean(centred * centred, axis=-1, keepdims=True)
        scaled = centred * lax.rsqrt(variance + 1e-05) * gain + offset
        normed_ref[place, :, span] = scaled.astype(jnp.bfloat16)


def norm(gain, offset, blocked, pieces, first, last):
    rows, cols, width = blocked.shape
    step = rows // 2
    shape = jax.ShapeDtypeStruct((2, step, WS, width), jnp.bfloat16)
    whole = pl.BlockSpec((width,), lambda i: (0,))
    in_specs = [whole, whole, pl.BlockSpec((1, cols, width), lambda i: (step + i, 0, 0))]
    in_specs += [pl.BlockSpec((1,) + p.shape[1:], lambda i: (i, 0, 0)) for p in pieces]
    out_spec = pl.BlockSpec((2, 1, WS, width), lambda i: (0, i, 0, 0))
    return pl.pallas_call(
        functools.partial(norm_kernel, (first, last)),
        grid=(step,),
        out_shape=(shape, shape),
        in_specs=in_specs,
        out_specs=(out_spec, out_spec),
        compiler_params=pltpu.CompilerParams(
            dimension_semantics=("arbitrary",), vmem_limit_bytes=8 << 20
        ),
        cost_estimate=pl.CostEstimate(
            flops=20 * rows * WS * width,
            transcendentals=0,
            bytes_accessed=8 * rows * WS * width,
        ),
    )(gain, offset, blocked, *pieces)


def pad_kernel(w_ref, out_ref):
    for h in range(w_ref.shape[2] // CHANNEL_PER_PART):
        part = w_ref[:, :, h * CHANNEL_PER_PART : (h + 1) * CHANNEL_PER_PART]
        empty = jnp.zeros(part.shape[:2] + (PADDED - CHANNEL_PER_PART,), part.dtype)
        out_ref[:, :, h * PADDED : (h + 1) * PADDED] = jnp.concatenate([part, empty], axis=2)


def pad_heads(weights):
    count, width, head_width = weights.shape
    padded = head_width // CHANNEL_PER_PART * PADDED
    tile = width // 4
    return pl.pallas_call(
        pad_kernel,
        grid=(count, 4),
        out_shape=jax.ShapeDtypeStruct((count, width, padded), weights.dtype),
        in_specs=[pl.BlockSpec((1, tile, head_width), lambda t, i: (t, i, 0))],
        out_specs=pl.BlockSpec((1, tile, padded), lambda t, i: (t, i, 0)),
        compiler_params=pltpu.CompilerParams(
            dimension_semantics=("arbitrary", "arbitrary"), vmem_limit_bytes=8 << 20
        ),
        cost_estimate=pl.CostEstimate(
            flops=count * width * padded * 64,
            transcendentals=0,
            bytes_accessed=2 * count * width * (padded + head_width),
        ),
    )(weights)


def attend_kernel(heads, lanes, window, scale_ref, w_ref, label_ref, *refs):
    x_refs, out_refs = refs[:lanes], refs[lanes : 2 * lanes]
    qkv, bias, columns = refs[2 * lanes :]
    me = lax.axis_index("seq")
    step = pl.program_id(0)
    chunk = bias.shape[0]

    for k in range(lanes):

        @pl.when(step == k)
        def _():
            rows = slice(k * chunk, (k + 1) * chunk)
            x = x_refs[k][...]
            columns[:, rows] = label_ref[window, me ^ k]
            for t in range(3):
                y = jnp.dot(x, w_ref[t], preferred_element_type=jnp.float32)
                if t == 2:
                    lane = lax.broadcasted_iota(jnp.int32, y.shape, 1)
                    y = jnp.where(lax.rem(lane, PADDED) == CHANNEL_PER_PART, 1.0, y)
                qkv[t, rows, :] = y.astype(jnp.bfloat16)

    for k in range(lanes):

        @pl.when(step == lanes + k)
        def _():
            rows = slice(k * chunk, (k + 1) * chunk)
            own = jnp.broadcast_to(label_ref[window, me ^ k], (8, chunk))
            own = jnp.transpose(own)[:, :1]
            bias[...] = jnp.where(own == columns[...], 0.0, -1e30)
            tempered = [scale_ref[h] * (LOG2E / math.sqrt(CHANNEL_PER_PART)) for h in range(heads)]
            for h in range(heads):
                cols = slice(h * PADDED, (h + 1) * PADDED)
                scores = lax.dot_general(
                    qkv[0, rows, cols],
                    qkv[1, :, cols],
                    (((1,), (1,)), ((), ())),
                    preferred_element_type=jnp.float32,
                )
                scores = scores + bias[...]
                row_max = jnp.max(scores, axis=-1, keepdims=True)
                numerators = jnp.exp2((scores - row_max) * tempered[h])
                summed = jnp.dot(
                    numerators.astype(jnp.bfloat16),
                    qkv[2, :, cols],
                    preferred_element_type=jnp.float32,
                )
                attended = summed / summed[:, CHANNEL_PER_PART : CHANNEL_PER_PART + 1]
                out_refs[k][:, h * CHANNEL_PER_PART : (h + 1) * CHANNEL_PER_PART] = attended[
                    :, :CHANNEL_PER_PART
                ].astype(jnp.bfloat16)


def attend(gathered, weights, labels, scale, window):
    lanes = len(gathered)
    chunk, width = gathered[0].shape
    heads = weights.shape[2] // PADDED
    pixels = lanes * chunk
    head_width = heads * CHANNEL_PER_PART
    flops = 2 * pixels * width * 3 * heads * PADDED + 4 * heads * pixels * pixels * PADDED
    once = pl.Buffered(1)
    return pl.pallas_call(
        functools.partial(attend_kernel, heads, lanes, window),
        grid=(2 * lanes,),
        out_shape=[jax.ShapeDtypeStruct((chunk, head_width), jnp.bfloat16)] * lanes,
        in_specs=[
            pl.BlockSpec(memory_space=pltpu.SMEM),
            pl.BlockSpec(weights.shape, lambda i: (0, 0, 0), pipeline_mode=once),
            pl.BlockSpec(labels.shape, lambda i: (0, 0, 0, 0), pipeline_mode=once),
        ]
        + [pl.BlockSpec((chunk, width), lambda i: (0, 0), pipeline_mode=once)] * lanes,
        out_specs=[pl.BlockSpec((chunk, head_width), lambda i: (0, 0))] * lanes,
        scratch_shapes=[
            pltpu.VMEM((3, pixels, heads * PADDED), jnp.bfloat16),
            pltpu.VMEM((chunk, pixels), jnp.float32),
            pltpu.VMEM((1, pixels), jnp.float32),
        ],
        compiler_params=pltpu.CompilerParams(
            dimension_semantics=("arbitrary",), vmem_limit_bytes=22 << 20
        ),
        cost_estimate=pl.CostEstimate(
            flops=flops,
            transcendentals=heads * pixels * pixels,
            bytes_accessed=2 * (pixels * (width + head_width) + weights.size),
        ),
    )(scale, weights, labels, *gathered)


def project_kernel(count, residual_ref, *refs):
    pieces, w_refs, out_ref = refs[:count], refs[count : 2 * count], refs[-1]
    rows, cols, tile = residual_ref.shape
    total = residual_ref[...].astype(jnp.float32).reshape(rows * cols, tile)
    for k in range(count):
        total += jnp.dot(pieces[k][...], w_refs[k][...], preferred_element_type=jnp.float32)
    out_ref[...] = total.reshape(rows, cols, tile).astype(jnp.bfloat16)


def project(residual, projection, pieces, window, window_count, previous):
    rows, cols, width = residual.shape
    count = len(pieces)
    tile = 512 if width % 512 == 0 else width
    in_specs = [pl.BlockSpec((rows, cols, tile), lambda i: (0, 0, i))]
    in_specs += [pl.BlockSpec(p.shape, lambda i: (0, 0)) for p in pieces]
    in_specs += [pl.BlockSpec((p.shape[0], tile), lambda i: (0, i)) for p in projection]
    operands = [residual, *pieces, *projection]
    aliases = {}
    if previous is not None:
        in_specs.append(pl.BlockSpec(memory_space=pl.ANY))
        aliases = {len(operands): 0}
        operands.append(previous)
    return pl.pallas_call(
        functools.partial(project_kernel, count),
        grid=(width // tile,),
        in_specs=in_specs,
        out_specs=pl.BlockSpec((rows, cols, tile), lambda i: (0, window, i)),
        out_shape=jax.ShapeDtypeStruct((rows, cols * window_count, width), jnp.bfloat16),
        input_output_aliases=aliases,
        compiler_params=pltpu.CompilerParams(
            dimension_semantics=("arbitrary",), vmem_limit_bytes=12 << 20
        ),
        cost_estimate=pl.CostEstimate(
            flops=2 * rows * cols * width * width,
            transcendentals=0,
            bytes_accessed=2 * (width * width + 3 * rows * cols * width),
        ),
    )(*operands)


def exchange(value, axis, mask):
    return lax.ppermute(value, axis, [(s, s ^ mask) for s in range(lax.axis_size(axis))])


def masks_of(count):
    return [1 << b for b in reversed(range(count.bit_length() - 1))]


def share(value, mask):
    rows = value.shape[0]
    if lax.axis_size("member") != 2 or rows % 2:
        return (exchange(value, "seq", mask),)
    start = lax.axis_index("member") * (rows // 2)
    sent = lax.dynamic_slice_in_dim(value, start, rows // 2, 0)
    return (exchange(sent, "seq", mask),)


def complete(received, rows):
    (direct,) = received
    if direct.shape[0] == rows:
        return direct
    relayed = exchange(direct, "member", 1)
    return jnp.where(
        lax.axis_index("member") == 0,
        jnp.concatenate([direct, relayed], axis=0),
        jnp.concatenate([relayed, direct], axis=0),
    )


def on_device(
    pixel_grid_input,
    mask_zone_labeling,
    standardize_multiplier,
    standardize_offset_vector,
    triple_projection_matrix,
    logit_scaling_per_part,
    final_projection_matrix,
):
    lanes = lax.axis_size("seq")
    me = lax.axis_index("seq")
    blocks = lax.axis_size("win")
    blocked = pixel_grid_input[0, :, 0]
    rows, cols, width = blocked.shape
    window_count = cols // WS
    half = WS // 2
    step = rows // 2
    chunk = rows * WS

    def fetch(value, source_of):
        return lax.ppermute(value, "win", [(source_of(d), d) for d in range(blocks)])

    def south(d):
        return d ^ 1

    def east(d):
        return (d + 2) % blocks

    def southeast(d):
        return ((d ^ 1) + 2) % blocks

    head_width = triple_projection_matrix.shape[2]
    heads = head_width // CHANNEL_PER_PART
    weights = pad_heads(triple_projection_matrix)
    labels = mask_zone_labeling[0].reshape(rows, lanes, window_count, WS).transpose(2, 1, 0, 3)
    labels = labels.reshape(window_count, lanes, 1, chunk).astype(jnp.float32)

    masks = masks_of(lanes)
    own_rows = final_projection_matrix.shape[0]
    first_share = share(final_projection_matrix, masks[0])
    shifted, normed, far = [], [], {}
    for window in range(window_count):
        first = window * WS + half
        last = min(first + WS, cols)
        pieces = [fetch(blocked[:step, first:last], south)]
        if last - first < WS:
            pieces.append(fetch(blocked[step:, :half], east))
            pieces.append(fetch(blocked[:step, :half], southeast))
        if window == 0:
            pieces[0], weights, labels = lax.optimization_barrier((pieces[0], weights, labels))
        if window == 1:
            pieces, far[0] = lax.optimization_barrier((pieces, far[0]))
        pixels, own = norm(
            standardize_multiplier, standardize_offset_vector, blocked, pieces, first, last
        )
        shifted.append(pixels.reshape(rows, WS, width))
        own = own.reshape(chunk, width)
        if window == 0:
            own, first_share = lax.optimization_barrier((own, first_share))
        normed.append(own)
        far[window] = exchange(own, "seq", masks[0])
    held = {0: final_projection_matrix, masks[0]: complete(first_share, own_rows)}
    for mask in masks[1:]:
        for k in list(held):
            if mask > 1:
                held[k ^ mask] = complete(share(held[k], mask), own_rows)
            else:
                held[k ^ mask] = exchange(held[k], "seq", mask)
    projection = [held[k] for k in range(lanes)]

    pieces = []
    before = None
    for window in range(window_count):
        held = {0: normed[window], masks[0]: far[window]}
        for mask in masks[1:]:
            if mask == 1 and before is not None:
                for k in list(held):
                    if k:
                        held[k] = lax.optimization_barrier((held[k], before))[0]
            for k in list(held):
                held[k ^ mask] = exchange(held[k], "seq", mask)
        gathered = [held[k] for k in range(lanes)]
        attended = attend(gathered, weights, labels, logit_scaling_per_part, window)
        before = attended[0]
        pieces.append(
            [exchange(attended[k], "seq", k) if k else attended[k] for k in range(lanes)]
        )

    result = None
    for window in range(window_count):
        result = project(
            shifted[window], projection, pieces[window], window, window_count, result
        )
    return result[None, :, None]


def solution(mesh):
    in_specs = (
        P(("member", "win"), None, "seq", None, None),
        P(("member", "win"), None, None),
        P(),
        P(),
        P(None, None, "seq"),
        P("seq"),
        P("seq", None),
    )
    out_specs = P(("member", "win"), None, "seq", None, None)
    return jax.shard_map(
        on_device, mesh=mesh, in_specs=in_specs, out_specs=out_specs, check_vma=False
    )
```
